32 devices in a mesh: rep: 8 (over y, x, core), row: 2 (over z_hi), col: 2 (over z_lo).
Axes of the slice: x: 2, y: 2, z: 4 (z_hi: 2, z_lo: 2; z = z_hi * 2 + z_lo), core: 2. Of those that a mesh axis runs over, the one named last changes fastest.
Arguments:
- activations: bfloat16 [2048, 2048], P(('rep', 'row'), 'col'), may hold values from -6 to 6
- out_grads: bfloat16 [2048, 2304], P(('rep', 'col'), 'row'), may hold values from -0.375 to 0.375
- error_buffer: float32 [16384, 2304], P(('rep', 'col'), 'row'), may hold values from -6 to 6
- right_factor: float32 [2304, 16], P('row'), may hold values from -6 to 6
Outputs:
- new_error: float32 [16384, 2304], P(('rep', 'col'), 'row')
- new_right: float32 [2304, 16], P('row')
The draws below stay inside these ranges and needn't reach their ends.
All inputs are finite; a program needn't handle non-finite values.
Results may differ from the reference program's by a relative error of at most 0.0003.
Values may be sent and summed in bfloat16 or wider, within the bound.
A program may use at most 64 MiB of HBM per device.

```python
import jax
import jax.numpy as jnp
from jax import lax

DR = 2048
DC = 2304
RANK = 16
TOK_REP = 256
TOKENS = 2048
ROWS_ALL = 16384
N_REP = 8


def steps_of(key, dims, shards, low, high):
    level = 1.0
    for position, shards_of in shards:
        heights = jax.random.uniform(jax.random.fold_in(jax.random.fold_in(key, 6), position), (shards_of,), jnp.float32, low / len(shards), high / len(shards))
        level = level * jnp.repeat(jnp.exp(heights), dims[position] // shards_of).reshape((-1,) + (1,) * (len(dims) - 1 - position))
    return level


def noise(rng, dims, deviation, bound, split=(), dtype=jnp.bfloat16):
    factor_of = steps_of(rng, dims, split, -0.22, 0.18) if split else 1.0
    result = jax.random.normal(rng, dims, jnp.float32) * deviation * factor_of
    return jnp.minimum(jnp.maximum(result, -bound), bound).astype(dtype)


def setup_inputs(seed: int = 0) -> dict:
    splits = jax.random.split(jax.random.key(seed), 5)
    activations = noise(splits[0], (TOKENS, DR), 1.0, 6.0, ((0, 16), (1, 2)))
    out_grads = noise(splits[1], (TOKENS, DC), TOK_REP ** -0.5, 0.375, ((0, 16), (1, 2)))
    error_buffer = noise(splits[2], (ROWS_ALL, DC), 1.0, 6.0, ((0, 16), (1, 2)), jnp.float32)
    right_factor = noise(splits[3], (DC, RANK), 1.0, 6.0, ((0, 2),), jnp.float32)
    return {"activations": activations, "out_grads": out_grads, "error_buffer": error_buffer, "right_factor": right_factor}


def reference(activations, out_grads, error_buffer, right_factor):
    highest = lax.Precision.HIGHEST
    acts = activations.reshape(N_REP, TOK_REP, DR)
    grads = out_grads.reshape(N_REP, TOK_REP, DC)
    errors = error_buffer.reshape(N_REP, DR, DC)

    def one_replica(items):
        act_block, grad_block, err_block = items
        product = lax.dot_general(act_block.astype(jnp.float32), grad_block.astype(jnp.float32), (((0,), (0,)), ((), ())), preferred_element_type=jnp.float32)
        return product + err_block
    target = lax.map(one_replica, (acts, grads, errors))
    left = jnp.einsum('rij,jk->ik', target, right_factor, precision=highest)
    gram = jnp.dot(left.T, left, precision=highest)
    lower = jnp.linalg.cholesky(gram)
    left_orth = jax.scipy.linalg.solve_triangular(lower, left.T, lower=True).T
    new_right = jnp.einsum('rij,ik->jk', target, left_orth, precision=highest) / N_REP
    approx = jnp.dot(left_orth, new_right.T, precision=highest)
    new_error = target - approx[None]
    return (new_error.reshape(N_REP * DR, DC), new_right)
```

```python
import functools

import jax
import jax.numpy as jnp
from jax import lax
from jax.experimental import pallas as pl
from jax.experimental.pallas import tpu as pltpu
from jax.sharding import PartitionSpec as P

MESH = pl.DeviceIdType.MESH
F32 = jnp.float32
BF16 = jnp.bfloat16
LANES = 128
SUB = 8
CHUNKS = 4


def plain_body(activations, out_grads, error_buffer, right_factor):
    highest = lax.Precision.HIGHEST
    gathered_acts = lax.all_gather(activations, "row", axis=0, tiled=True)
    gathered_grads = lax.all_gather(out_grads, "col", axis=0, tiled=True)
    product = lax.dot_general(
        gathered_acts, gathered_grads, (((0,), (0,)), ((), ())), preferred_element_type=F32
    )
    target = product + error_buffer
    replicas = lax.axis_size("rep")
    left_part = lax.psum_scatter(
        jnp.dot(target, right_factor, precision=highest), "rep", scatter_dimension=0, tiled=True
    )
    left_part = lax.psum(left_part, "row")
    gram = lax.psum(jnp.dot(left_part.T, left_part, precision=highest), ("rep", "col"))
    lower = jnp.linalg.cholesky(gram)
    orth_part = jax.scipy.linalg.solve_triangular(lower, left_part.T, lower=True).T
    left_orth = lax.all_gather(orth_part, "rep", axis=0, tiled=True)
    right_part = lax.psum_scatter(
        lax.dot_general(
            target, left_orth, (((0,), (0,)), ((), ())), precision=highest, preferred_element_type=F32
        ),
        "rep",
        scatter_dimension=0,
        tiled=True,
    )
    right_part = lax.psum(right_part, "col") / replicas
    new_right = lax.all_gather(right_part, "rep", axis=0, tiled=True)
    approx = jnp.dot(left_orth, new_right.T, precision=highest)
    return (target - approx, new_right)


def split2(x):
    hi = x.astype(BF16)
    lo = (x - hi.astype(F32)).astype(BF16)
    return hi, lo


def dot(a, b, ca, cb, precision=None):
    return lax.dot_general(a, b, (((ca,), (cb,)), ((), ())), preferred_element_type=F32, precision=precision)


def factor_kernel(
    nrep, nrow, ncol, owners, tpd,
    acts, grads, err, right,
    t_out, los, nrs, nrt,
    e_buf, t_hi, t_lo, a_all, g_all, gr_own, gr_all,
    lp, l_rx, l_own, l_row, lag, gram_all, w_tx, w_rx, w_own, w_col, wag,
    esem, tsem, loc_sem, a_ss, a_rs, g_ss, g_rs, gr_ss, gr_rs,
    l_ss, l_rs, lr_ss, lr_rs, la_ss, la_rs, gm_ss, gm_rs,
    w_ss, w_rs, wc_ss, wc_rs, wa_ss, wa_rs,
):
    rep, row, col = lax.axis_index("rep"), lax.axis_index("row"), lax.axis_index("col")
    rows, cols = e_buf.shape
    rank = right.shape[1]
    chunk = rows // CHUNKS
    highest = lax.Precision.HIGHEST
    sent = []

    def remote(src, dst, ss, rs, where):
        return pltpu.make_async_remote_copy(
            src_ref=src, dst_ref=dst, send_sem=ss, recv_sem=rs, device_id=where, device_id_type=MESH
        )

    def turn(i, k, n):
        return lax.rem(i + k, n)

    barrier = pltpu.get_barrier_semaphore()
    for k in range(1, nrep):
        pl.semaphore_signal(barrier, inc=1, device_id={"rep": turn(rep, k, nrep)}, device_id_type=MESH)
    for i in range(nrow):
        for j in range(ncol):
            if i or j:
                pl.semaphore_signal(
                    barrier, inc=1,
                    device_id={"row": turn(row, i, nrow), "col": turn(col, j, ncol)},
                    device_id_type=MESH,
                )

    loads = []
    for c in range(CHUNKS):
        part = pl.ds(c * chunk, chunk)
        loads.append(pltpu.make_async_copy(err.at[part], e_buf.at[part], esem.at[c]))
        loads[-1].start()
    own_a = pltpu.make_async_copy(acts, a_all.at[row], loc_sem.at[0])
    own_g = pltpu.make_async_copy(grads, g_all.at[col], loc_sem.at[1])
    own_a.start()
    own_g.start()

    right_t = right[...].T
    r_hi, r_lo = split2(right_t)
    r_two = jnp.concatenate([r_hi, r_lo], axis=0)
    gr2 = dot(r_two, grads[...], 1, 1)
    gr_own[...] = gr2[:rank] + gr2[rank:]

    pl.semaphore_wait(barrier, nrep - 1 + nrow * ncol - 1)

    gr_copies = []
    for j in range(ncol):
        cp = remote(gr_own, gr_all.at[row], gr_ss.at[j], gr_rs.at[row], {"row": col, "col": j})
        is_self = jnp.logical_and(row == col, col == j)
        gr_copies.append((cp, is_self))

        @pl.when(jnp.logical_not(is_self))
        def _():
            cp.start()

    @pl.when(row == col)
    def _():
        gr_all[row] = gr_own[...]

    ta, tg = acts.shape[0] // 2, grads.shape[0] // 2
    bulk = []
    for half in range(2):
        part = []
        for k in range(1, nrow):
            s = pl.ds(half * ta, ta)
            part.append(remote(acts.at[s], a_all.at[row, s], a_ss.at[half, k], a_rs.at[half, k], {"row": turn(row, k, nrow)}))
        for k in range(1, ncol):
            s = pl.ds(half * tg, tg)
            part.append(remote(grads.at[s], g_all.at[col, s], g_ss.at[half, k], g_rs.at[half, k], {"col": turn(col, k, ncol)}))
        bulk.append(part)
    for cp in bulk[0]:
        cp.start()

    pieces = []
    for c in range(CHUNKS):
        loads[c].wait()
        hi, lo = split2(e_buf[pl.ds(c * chunk, chunk), :])
        two = dot(r_two, hi, 1, 1)
        pieces.append(two[:rank] + two[rank:] + dot(r_hi, lo, 1, 1))
    for i in range(nrow):
        @pl.when(jnp.logical_not(jnp.logical_and(row == col, row == i)))
        def _():
            remote(gr_own, gr_all.at[i], gr_ss.at[0], gr_rs.at[i], {"row": col}).wait_recv()
    gr = gr_all[0]
    for i in range(1, nrow):
        gr = gr + gr_all[i]
    gr_hi, gr_lo = split2(gr)
    two = dot(jnp.concatenate([gr_hi, gr_lo], axis=0), acts[...], 1, 0)
    part_left = jnp.concatenate(pieces, axis=1) + two[:rank] + two[rank:]
    width = rows // nrep
    for k in range(nrep):
        lp[k] = part_left[:, k * width:(k + 1) * width]

    copies = []
    for k in range(1, nrep):
        to = turn(rep, k, nrep)
        cp = remote(lp.at[to], l_rx.at[rep], l_ss.at[k], l_rs.at[k], {"rep": to})
        cp.start()
        copies.append(cp)
    sent += copies
    total = lp[rep]
    for k, cp in enumerate(copies, 1):
        cp.wait_recv()
        total = total + l_rx[turn(rep, nrep - k, nrep)]
    l_own[...] = total
    copies = []
    for k in range(1, nrow):
        cp = remote(l_own, l_row.at[row], lr_ss.at[k], lr_rs.at[k], {"row": turn(row, k, nrow)})
        cp.start()
        copies.append(cp)
    sent += copies
    for cp in bulk[1]:
        cp.start()
    l_row[row] = total
    for cp in copies:
        cp.wait_recv()
    total = l_row[0]
    for i in range(1, nrow):
        total = total + l_row[i]
    lag[rep] = total
    copies = []
    for k in range(1, nrep):
        cp = remote(lag.at[rep], lag.at[rep], la_ss.at[k], la_rs.at[k], {"rep": turn(rep, k, nrep)})
        cp.start()
        copies.append(cp)
    sent += copies
    for cp in copies:
        cp.wait_recv()
    left = jnp.concatenate([lag[k] for k in range(nrep)], axis=1)
    l_hi, l_lo = split2(left)
    l_two = jnp.concatenate([l_hi, l_lo], axis=0)

    gram_all[col] = jnp.zeros(gram_all.shape[1:], F32)
    gram_all[col, :, 0:rank] = dot(left, left, 1, 1, highest)
    gram_copies = []
    for k in range(1, ncol):
        cp = remote(gram_all.at[col], gram_all.at[col], gm_ss.at[k], gm_rs.at[k], {"col": turn(col, k, ncol)})
        cp.start()
        gram_copies.append(cp)
    sent += gram_copies

    own_a.wait()
    own_g.wait()
    for part in bulk:
        for cp in part:
            cp.wait_recv()
    a = a_all[...].reshape(nrow * acts.shape[0], rows)
    g = g_all[...].reshape(ncol * grads.shape[0], cols)
    stores = []
    w = jnp.zeros((rank, cols), F32)
    for c in range(CHUNKS):
        part = pl.ds(c * chunk, chunk)
        t = dot(a[:, c * chunk:(c + 1) * chunk], g, 0, 0) + e_buf[part, :]
        e_buf[part, :] = t
        stores.append(pltpu.make_async_copy(e_buf.at[part], t_out.at[part], tsem.at[c]))
        stores[-1].start()
        hi, lo = split2(t)
        two = dot(l_two[:, c * chunk:(c + 1) * chunk], hi, 1, 0)
        w = w + two[:rank] + two[rank:] + dot(l_hi[:, c * chunk:(c + 1) * chunk], lo, 1, 0)
    lane_tiles = cols // LANES
    tiles = (rank // SUB) * lane_tiles
    for t in range(owners * tpd):
        if t < tiles:
            h, l = divmod(t, lane_tiles)
            w_tx[t // tpd, t % tpd] = w[h * SUB:(h + 1) * SUB, l * LANES:(l + 1) * LANES]
        else:
            w_tx[t // tpd, t % tpd] = jnp.zeros((SUB, LANES), F32)

    copies = []
    for k in range(1, nrep):
        to = turn(rep, k, nrep)
        keep = to < owners
        slot = jnp.minimum(to, owners - 1)
        cp = remote(w_tx.at[slot], w_rx.at[rep], w_ss.at[k], w_rs.at[k], {"rep": to})
        copies.append((cp, keep))

        @pl.when(keep)
        def _():
            cp.start()

    for cp in gram_copies:
        cp.wait_recv()
    gram = gram_all[0]
    for j in range(1, ncol):
        gram = gram + gram_all[j]
    gram = gram[:, 0:rank]
    ri = lax.broadcasted_iota(jnp.int32, (rank, rank), 0)
    ci = lax.broadcasted_iota(jnp.int32, (rank, rank), 1)
    r1 = lax.broadcasted_iota(jnp.int32, (rank, 1), 0)
    inv = jnp.where(ri == ci, 1.0, 0.0).astype(F32)
    for j in range(rank):
        f = jnp.where(r1 > j, gram[:, j:j + 1] / gram[j:j + 1, j:j + 1], 0.0)
        inv = inv - f * inv[j:j + 1, :]
        gram = gram - f * gram[j:j + 1, :]
    diag = jnp.sum(jnp.where(ri == ci, gram, 0.0), axis=1, keepdims=True)
    inv = inv / jnp.sqrt(diag)
    lo_t = dot(inv, left, 1, 0, highest)
    o_hi, o_lo = split2(lo_t)
    los[...] = jnp.concatenate([o_hi, o_hi, o_lo], axis=0)

    mine = rep < owners

    @pl.when(mine)
    def _():
        total = w_tx[jnp.minimum(rep, owners - 1)]
        for k, (cp, keep) in enumerate(copies, 1):
            cp.wait_recv()
            total = total + w_rx[turn(rep, nrep - k, nrep)]
        w_own[...] = total
        ex = []
        for k in range(1, ncol):
            cp = remote(w_own, w_col.at[col], wc_ss.at[k], wc_rs.at[k], {"col": turn(col, k, ncol)})
            cp.start()
            ex.append(cp)
        w_col[col] = total
        for cp in ex:
            cp.wait_recv()
        total = w_col[0]
        for j in range(1, ncol):
            total = total + w_col[j]
        slot = jnp.minimum(rep, owners - 1)
        wag[slot] = total
        for k in range(1, nrep):
            remote(wag.at[slot], wag.at[slot], wa_ss.at[k], wa_rs.at[k], {"rep": turn(rep, k, nrep)}).start()
        for cp in ex:
            cp.wait_send()

    for k in range(1, nrep):
        @pl.when(turn(rep, nrep - k, nrep) < owners)
        def _():
            remote(wag.at[0], wag.at[0], wa_ss.at[k], wa_rs.at[k], {"rep": turn(rep, k, nrep)}).wait_recv()
    halves = []
    for h in range(rank // SUB):
        ts = [h * lane_tiles + l for l in range(lane_tiles)]
        halves.append(jnp.concatenate([wag[t // tpd, t % tpd] for t in ts], axis=1))
    w_all = jnp.concatenate(halves, axis=0)
    nr = dot(inv, w_all, 1, 0, highest) / nrep
    nrt[...] = nr
    n_hi, n_lo = split2(nr)
    nrs[...] = jnp.concatenate([n_hi, n_lo, n_hi], axis=0)

    for cp, is_self in gr_copies:
        @pl.when(jnp.logical_not(is_self))
        def _():
            cp.wait_send()
    for cp in sent:
        cp.wait_send()
    for part in bulk:
        for cp in part:
            cp.wait_send()
    for cp, keep in copies:
        @pl.when(keep)
        def _():
            cp.wait_send()

    @pl.when(mine)
    def _():
        for k in range(1, nrep):
            remote(wag.at[0], wag.at[0], wa_ss.at[k], wa_rs.at[k], {"rep": turn(rep, k, nrep)}).wait_send()
    for cp in stores:
        cp.wait()


def finish_kernel(t, los, nrs, nrt, out, right_out):
    out[...] = t[...] - dot(los[...], nrs[...], 0, 0)

    @pl.when(pl.program_id(0) == 0)
    def _():
        right_out[...] = nrt[...].T


def kernel_body(nrep, nrow, ncol, activations, out_grads, error_buffer, right_factor):
    rows, cols = error_buffer.shape
    rank = right_factor.shape[1]
    ta, tg = activations.shape[0], out_grads.shape[0]
    tiles = (rank // SUB) * (cols // LANES)
    tpd = -(-tiles // nrep)
    owners = -(-tiles // tpd)
    width = rows // nrep
    vmem = pl.BlockSpec(memory_space=pltpu.VMEM)
    hbm = pl.BlockSpec(memory_space=pl.ANY)
    dma = lambda *s: pltpu.SemaphoreType.DMA(s)
    target, los, nrs, nrt = pl.pallas_call(
        functools.partial(factor_kernel, nrep, nrow, ncol, owners, tpd),
        out_shape=(
            jax.ShapeDtypeStruct((rows, cols), F32),
            jax.ShapeDtypeStruct((3 * rank, rows), BF16),
            jax.ShapeDtypeStruct((3 * rank, cols), BF16),
            jax.ShapeDtypeStruct((rank, cols), F32),
        ),
        in_specs=[vmem, vmem, hbm, vmem],
        out_specs=(hbm, vmem, vmem, vmem),
        scratch_shapes=[
            pltpu.VMEM((rows, cols), F32),
            pltpu.VMEM((SUB, LANES), BF16),
            pltpu.VMEM((SUB, LANES), BF16),
            pltpu.VMEM((nrow, ta, rows), BF16),
            pltpu.VMEM((ncol, tg, cols), BF16),
            pltpu.VMEM((rank, tg), F32),
            pltpu.VMEM((nrow, rank, tg), F32),
            pltpu.VMEM((nrep, rank, width), F32),
            pltpu.VMEM((nrep, rank, width), F32),
            pltpu.VMEM((rank, width), F32),
            pltpu.VMEM((nrow, rank, width), F32),
            pltpu.VMEM((nrep, rank, width), F32),
            pltpu.VMEM((ncol, rank, LANES), F32),
            pltpu.VMEM((owners, tpd, SUB, LANES), F32),
            pltpu.VMEM((nrep, tpd, SUB, LANES), F32),
            pltpu.VMEM((tpd, SUB, LANES), F32),
            pltpu.VMEM((ncol, tpd, SUB, LANES), F32),
            pltpu.VMEM((owners, tpd, SUB, LANES), F32),
            dma(CHUNKS), dma(CHUNKS), dma(2),
            dma(2, nrow), dma(2, nrow), dma(2, ncol), dma(2, ncol),
            dma(ncol), dma(nrow),
            dma(nrep), dma(nrep), dma(nrow), dma(nrow), dma(nrep), dma(nrep), dma(ncol), dma(ncol),
            dma(nrep), dma(nrep), dma(ncol), dma(ncol), dma(nrep), dma(nrep),
        ],
        compiler_params=pltpu.CompilerParams(collective_id=0, has_side_effects=True),
        name="factors",
    )(activations, out_grads, error_buffer, right_factor)
    steps = 8
    block = rows // steps
    return pl.pallas_call(
        finish_kernel,
        grid=(steps,),
        out_shape=(
            jax.ShapeDtypeStruct((rows, cols), F32),
            jax.ShapeDtypeStruct((cols, rank), F32),
        ),
        in_specs=[
            pl.BlockSpec((block, cols), lambda i: (i, 0)),
            pl.BlockSpec((3 * rank, block), lambda i: (0, i)),
            pl.BlockSpec((3 * rank, cols), lambda i: (0, 0)),
            pl.BlockSpec((rank, cols), lambda i: (0, 0)),
        ],
        out_specs=(
            pl.BlockSpec((block, cols), lambda i: (i, 0)),
            pl.BlockSpec((cols, rank), lambda i: (0, 0)),
        ),
        name="finish",
    )(target, los, nrs, nrt)


def body(activations, out_grads, error_buffer, right_factor):
    nrep, nrow, ncol = (lax.axis_size(a) for a in ("rep", "row", "col"))
    rows, cols = error_buffer.shape
    rank = right_factor.shape[1]
    fits = (
        nrep <= 16
        and nrow == ncol
        and activations.shape[0] % LANES == 0
        and rows % (nrep * LANES) == 0
        and rows % (8 * LANES) == 0
        and cols % LANES == 0
        and rank % 16 == 0
        and rank <= LANES
        and rows * cols * 4 <= 2**23
    )
    if not fits:
        return plain_body(activations, out_grads, error_buffer, right_factor)
    return kernel_body(nrep, nrow, ncol, activations, out_grads, error_buffer, right_factor)


def solution(mesh):
    return jax.shard_map(
        body,
        mesh=mesh,
        in_specs=(
            P(("rep", "row"), "col"),
            P(("rep", "col"), "row"),
            P(("rep", "col"), "row"),
            P("row", None),
        ),
        out_specs=(P(("rep", "col"), "row"), P("row", None)),
        check_vma=False,
    )
```

```python
import functools

import jax
import jax.numpy as jnp
from jax import lax
from jax.experimental import pallas as pl
from jax.experimental.pallas import tpu as pltpu
from jax.sharding import PartitionSpec as P

MESH = pl.DeviceIdType.MESH
F32 = jnp.float32
BF16 = jnp.bfloat16
LANES = 128
SUB = 8
CHUNKS = 4
QUARTERS = 4
GRANT = 24 * 2**20


def plain_body(activations, out_grads, error_buffer, right_factor):
    highest = lax.Precision.HIGHEST
    gathered_acts = lax.all_gather(activations, "row", axis=0, tiled=True)
    gathered_grads = lax.all_gather(out_grads, "col", axis=0, tiled=True)
    product = lax.dot_general(
        gathered_acts, gathered_grads, (((0,), (0,)), ((), ())), preferred_element_type=F32
    )
    target = product + error_buffer
    replicas = lax.axis_size("rep")
    left_part = lax.psum_scatter(
        jnp.dot(target, right_factor, precision=highest), "rep", scatter_dimension=0, tiled=True
    )
    left_part = lax.psum(left_part, "row")
    gram = lax.psum(jnp.dot(left_part.T, left_part, precision=highest), ("rep", "col"))
    lower = jnp.linalg.cholesky(gram)
    orth_part = jax.scipy.linalg.solve_triangular(lower, left_part.T, lower=True).T
    left_orth = lax.all_gather(orth_part, "rep", axis=0, tiled=True)
    right_part = lax.psum_scatter(
        lax.dot_general(
            target, left_orth, (((0,), (0,)), ((), ())), precision=highest, preferred_element_type=F32
        ),
        "rep",
        scatter_dimension=0,
        tiled=True,
    )
    right_part = lax.psum(right_part, "col") / replicas
    new_right = lax.all_gather(right_part, "rep", axis=0, tiled=True)
    approx = jnp.dot(left_orth, new_right.T, precision=highest)
    return (target - approx, new_right)


def split2(x):
    hi = x.astype(BF16)
    lo = (x - hi.astype(F32)).astype(BF16)
    return hi, lo


def dot(a, b, ca, cb, precision=None):
    return lax.dot_general(a, b, (((ca,), (cb,)), ((), ())), preferred_element_type=F32, precision=precision)


def factor_kernel(
    nrep, nrow, ncol, owners, tpd,
    acts_in, grads_in, err, right_in,
    target, los, nrs, nrt,
    e_hi, e_lo, right_t, a_all, g_all, gr_own, gr_all, la_own, la_all,
    lp, l_rx, l_own, l_row, lag, gram_all, w_tx, w_rx, w_own, w_col, wag,
    esem, loc_sem, a_ss, a_rs, g_ss, g_rs, gr_ss, gr_rs, lt_ss, lt_rs,
    l_ss, l_rs, lr_ss, lr_rs, la_ss, la_rs, gm_ss, gm_rs,
    w_ss, w_rs, wc_ss, wc_rs, wa_ss, wa_rs,
):
    rep, row, col = lax.axis_index("rep"), lax.axis_index("row"), lax.axis_index("col")
    rows, cols = target.shape
    rank = right_t.shape[0]
    chunk = rows // CHUNKS
    highest = lax.Precision.HIGHEST
    sent = []

    def remote(src, dst, ss, rs, where):
        return pltpu.make_async_remote_copy(
            src_ref=src, dst_ref=dst, send_sem=ss, recv_sem=rs, device_id=where, device_id_type=MESH
        )

    def turn(i, k, n):
        return lax.rem(i + k, n)

    barrier = pltpu.get_barrier_semaphore()
    for i in range(nrow):
        for j in range(ncol):
            if i or j:
                pl.semaphore_signal(
                    barrier, inc=1,
                    device_id={"row": turn(row, i, nrow), "col": turn(col, j, ncol)},
                    device_id_type=MESH,
                )
    for k in range(1, nrep):
        pl.semaphore_signal(barrier, inc=1, device_id={"rep": turn(rep, k, nrep)}, device_id_type=MESH)

    acts, grads = a_all.at[row], g_all.at[col]
    own_r = pltpu.make_async_copy(right_in, right_t, loc_sem.at[0])
    own_g = pltpu.make_async_copy(grads_in, grads, loc_sem.at[1])
    own_a = pltpu.make_async_copy(acts_in, acts, loc_sem.at[2])
    own_r.start()
    own_g.start()
    loads = []
    for c in range(CHUNKS):
        part = pl.ds(c * chunk, chunk)
        loads.append(pltpu.make_async_copy(err.at[part], target.at[part], esem.at[c]))
        loads[-1].start()
    own_a.start()
    own_r.wait()
    own_g.wait()
    r_hi, r_lo = split2(right_t[...])
    r_two = jnp.concatenate([r_hi, r_lo], axis=0)
    gr2 = dot(r_two, grads[...], 1, 1)
    gr_own[...] = gr2[:rank] + gr2[rank:]

    pieces = []

    def error_term(c):
        loads[c].wait()
        part = pl.ds(c * chunk, chunk)
        hi, lo = split2(target[part, :])
        e_hi[part, :] = hi
        e_lo[part, :] = lo
        two = dot(r_two, hi, 1, 1)
        pieces.append(two[:rank] + two[rank:] + dot(r_hi, lo, 1, 1))

    early = CHUNKS // 2
    for c in range(early):
        error_term(c)
    own_a.wait()

    pl.semaphore_wait(barrier, nrep - 1 + nrow * ncol - 1)

    gr_copies = []
    for j in range(ncol):
        cp = remote(gr_own, gr_all.at[row], gr_ss.at[j], gr_rs.at[row], {"row": col, "col": j})
        is_self = jnp.logical_and(row == col, col == j)
        gr_copies.append((cp, is_self))

        @pl.when(jnp.logical_not(is_self))
        def _():
            cp.start()

    @pl.when(row == col)
    def _():
        gr_all[row] = gr_own[...]

    ta, tg = acts.shape[0] // QUARTERS, grads.shape[0] // QUARTERS
    bulk = []
    for q in range(QUARTERS):
        for k in range(1, nrow):
            s = pl.ds(q * ta, ta)
            bulk.append(remote(a_all.at[row, s], a_all.at[row, s], a_ss.at[q, k], a_rs.at[q, k], {"row": turn(row, k, nrow)}))
        for k in range(1, ncol):
            s = pl.ds(q * tg, tg)
            bulk.append(remote(g_all.at[col, s], g_all.at[col, s], g_ss.at[q, k], g_rs.at[q, k], {"col": turn(col, k, ncol)}))
    per = nrow + ncol - 2
    for cp in bulk[:2 * per]:
        cp.start()

    for c in range(early, CHUNKS):
        error_term(c)
    for i in range(nrow):
        @pl.when(jnp.logical_not(jnp.logical_and(row == col, row == i)))
        def _():
            remote(gr_own, gr_all.at[i], gr_ss.at[0], gr_rs.at[i], {"row": col}).wait_recv()
    gr = gr_all[0]
    for i in range(1, nrow):
        gr = gr + gr_all[i]
    gr_hi, gr_lo = split2(gr)
    two = dot(jnp.concatenate([gr_hi, gr_lo], axis=0), acts[...], 1, 0)
    part_left = jnp.concatenate(pieces, axis=1) + two[:rank] + two[rank:]
    width = rows // nrep
    for k in range(nrep):
        lp[k] = part_left[:, k * width:(k + 1) * width]

    copies = []
    for k in range(1, nrep):
        to = turn(rep, k, nrep)
        cp = remote(lp.at[to], l_rx.at[rep], l_ss.at[k], l_rs.at[k], {"rep": to})
        cp.start()
        copies.append(cp)
    sent += copies
    total = lp[rep]
    for k, cp in enumerate(copies, 1):
        cp.wait_recv()
        total = total + l_rx[turn(rep, nrep - k, nrep)]
    l_own[...] = total
    copies = []
    for k in range(1, nrow):
        cp = remote(l_own, l_row.at[row], lr_ss.at[k], lr_rs.at[k], {"row": turn(row, k, nrow)})
        cp.start()
        copies.append(cp)
    sent += copies
    for cp in bulk[2 * per:3 * per]:
        cp.start()
    l_row[row] = total
    for cp in copies:
        cp.wait_recv()
    total = l_row[0]
    for i in range(1, nrow):
        total = total + l_row[i]
    lag[rep] = total
    copies = []
    for k in range(1, nrep):
        cp = remote(lag.at[rep], lag.at[rep], la_ss.at[k], la_rs.at[k], {"rep": turn(rep, k, nrep)})
        cp.start()
        copies.append(cp)
    sent += copies
    for cp in copies:
        cp.wait_recv()
    left = jnp.concatenate([lag[k] for k in range(nrep)], axis=1)
    l_hi, l_lo = split2(left)
    l_two = jnp.concatenate([l_hi, l_lo], axis=0)

    la2 = dot(l_two, acts[...], 1, 1)
    la_own[...] = la2[:rank] + la2[rank:]
    lt_copies = []
    for i in range(nrow):
        cp = remote(la_own, la_all.at[col], lt_ss.at[i], lt_rs.at[col], {"row": i, "col": row})
        is_self = jnp.logical_and(row == col, row == i)
        lt_copies.append((cp, is_self))

        @pl.when(jnp.logical_not(is_self))
        def _():
            cp.start()

    @pl.when(row == col)
    def _():
        la_all[col] = la_own[...]

    gram_all[col] = jnp.zeros(gram_all.shape[1:], F32)
    gram_all[col, :, 0:rank] = dot(left, left, 1, 1, highest)
    gram_copies = []
    for k in range(1, ncol):
        cp = remote(gram_all.at[col], gram_all.at[col], gm_ss.at[k], gm_rs.at[k], {"col": turn(col, k, ncol)})
        cp.start()
        gram_copies.append(cp)
    sent += gram_copies
    for cp in bulk[3 * per:]:
        cp.start()

    two = dot(l_two, e_hi[...], 1, 0)
    w = two[:rank] + two[rank:] + dot(l_hi, e_lo[...], 1, 0)
    for j in range(ncol):
        @pl.when(jnp.logical_not(jnp.logical_and(row == col, col == j)))
        def _():
            remote(la_own, la_all.at[j], lt_ss.at[0], lt_rs.at[j], {"col": row}).wait_recv()
    la = la_all[0]
    for j in range(1, ncol):
        la = la + la_all[j]
    la_hi, la_lo = split2(la)
    two = dot(jnp.concatenate([la_hi, la_lo], axis=0), grads[...], 1, 0)
    w = w + two[:rank] + two[rank:]
    lane_tiles = cols // LANES
    tiles = (rank // SUB) * lane_tiles
    for t in range(owners * tpd):
        if t < tiles:
            h, l = divmod(t, lane_tiles)
            w_tx[t // tpd, t % tpd] = w[h * SUB:(h + 1) * SUB, l * LANES:(l + 1) * LANES]
        else:
            w_tx[t // tpd, t % tpd] = jnp.zeros((SUB, LANES), F32)

    copies = []
    for k in range(1, nrep):
        to = turn(rep, k, nrep)
        keep = to < owners
        slot = jnp.minimum(to, owners - 1)
        cp = remote(w_tx.at[slot], w_rx.at[rep], w_ss.at[k], w_rs.at[k], {"rep": to})
        copies.append((cp, keep))

        @pl.when(keep)
        def _():
            cp.start()

    for cp in gram_copies:
        cp.wait_recv()
    gram = gram_all[0]
    for j in range(1, ncol):
        gram = gram + gram_all[j]
    gram = gram[:, 0:rank]
    ri = lax.broadcasted_iota(jnp.int32, (rank, rank), 0)
    ci = lax.broadcasted_iota(jnp.int32, (rank, rank), 1)
    r1 = lax.broadcasted_iota(jnp.int32, (rank, 1), 0)
    inv = jnp.where(ri == ci, 1.0, 0.0).astype(F32)
    for j in range(rank):
        f = jnp.where(r1 > j, gram[:, j:j + 1] / gram[j:j + 1, j:j + 1], 0.0)
        inv = inv - f * inv[j:j + 1, :]
        gram = gram - f * gram[j:j + 1, :]
    diag = jnp.sum(jnp.where(ri == ci, gram, 0.0), axis=1, keepdims=True)
    inv = inv / jnp.sqrt(diag)

    mine = rep < owners
    own_slot = jnp.minimum(rep, owners - 1)
    ex = [
        remote(w_own, w_col.at[col], wc_ss.at[k], wc_rs.at[k], {"col": turn(col, k, ncol)})
        for k in range(1, ncol)
    ]
    gather = [
        remote(wag.at[own_slot], wag.at[own_slot], wa_ss.at[k], wa_rs.at[k], {"rep": turn(rep, k, nrep)})
        for k in range(1, nrep)
    ]

    @pl.when(mine)
    def _():
        total = w_tx[own_slot]
        for k, (cp, keep) in enumerate(copies, 1):
            cp.wait_recv()
            total = total + w_rx[turn(rep, nrep - k, nrep)]
        w_own[...] = total
        w_col[col] = total
        for cp in ex:
            cp.start()

    for cp in bulk:
        cp.wait_recv()

    def target_term(c):
        part = pl.ds(c * chunk, chunk)
        a = a_all[:, :, c * chunk:(c + 1) * chunk].reshape(nrow * acts.shape[0], chunk)
        g = g_all[...].reshape(ncol * grads.shape[0], cols)
        target[part, :] = dot(a, g, 0, 0) + target[part, :]

    for c in range(early):
        target_term(c)

    @pl.when(mine)
    def _():
        for cp in ex:
            cp.wait_recv()
        total = w_col[0]
        for j in range(1, ncol):
            total = total + w_col[j]
        wag[own_slot] = total
        for cp in gather:
            cp.start()

    lo_t = dot(inv, left, 1, 0, highest)
    o_hi, o_lo = split2(lo_t)
    los[...] = jnp.concatenate([o_hi, o_hi, o_lo], axis=0)
    for c in range(early, CHUNKS):
        target_term(c)

    for k in range(1, nrep):
        @pl.when(turn(rep, nrep - k, nrep) < owners)
        def _():
            gather[k - 1].wait_recv()
    halves = []
    for h in range(rank // SUB):
        ts = [h * lane_tiles + l for l in range(lane_tiles)]
        halves.append(jnp.concatenate([wag[t // tpd, t % tpd] for t in ts], axis=1))
    w_all = jnp.concatenate(halves, axis=0)
    nr = dot(inv, w_all, 1, 0, highest) / nrep
    nrt[...] = nr
    n_hi, n_lo = split2(nr)
    nrs[...] = jnp.concatenate([n_hi, n_lo, n_hi], axis=0)

    for cp, is_self in gr_copies + lt_copies:
        @pl.when(jnp.logical_not(is_self))
        def _():
            cp.wait_send()
    for cp in sent + bulk:
        cp.wait_send()
    for cp, keep in copies:
        @pl.when(keep)
        def _():
            cp.wait_send()

    @pl.when(mine)
    def _():
        for cp in ex + gather:
            cp.wait_send()


def finish_kernel(t, los, nrs, nrt, out, right_out, buf, sem):
    rows = t.shape[0]
    steps = sem.shape[0]
    block = rows // steps
    stores = []
    for c in range(steps):
        part = pl.ds(c * block, block)
        buf[part, :] = t[part, :] - dot(los[:, c * block:(c + 1) * block], nrs[...], 0, 0)
        stores.append(pltpu.make_async_copy(buf.at[part], out.at[part], sem.at[c]))
        stores[-1].start()
    right_out[...] = nrt[...]
    for cp in stores:
        cp.wait()


def kernel_body(nrep, nrow, ncol, activations, out_grads, error_buffer, right_factor):
    rows, cols = error_buffer.shape
    rank = right_factor.shape[1]
    ta, tg = activations.shape[0], out_grads.shape[0]
    tiles = (rank // SUB) * (cols // LANES)
    tpd = -(-tiles // nrep)
    owners = -(-tiles // tpd)
    width = rows // nrep
    vmem = pl.BlockSpec(memory_space=pltpu.VMEM)
    hbm = pl.BlockSpec(memory_space=pltpu.HBM)
    dma = lambda *s: pltpu.SemaphoreType.DMA(s)
    target, los, nrs, nrt = pl.pallas_call(
        functools.partial(factor_kernel, nrep, nrow, ncol, owners, tpd),
        out_shape=(
            pltpu.VMEM((rows, cols), F32),
            pltpu.VMEM((3 * rank, rows), BF16),
            pltpu.VMEM((3 * rank, cols), BF16),
            pltpu.VMEM((rank, cols), F32),
        ),
        in_specs=[hbm] * 4,
        out_specs=(vmem, vmem, vmem, vmem),
        scratch_shapes=[
            pltpu.VMEM((rows, cols), BF16),
            pltpu.VMEM((rows, cols), BF16),
            pltpu.VMEM((rank, cols), F32),
            pltpu.VMEM((nrow, ta, rows), BF16),
            pltpu.VMEM((ncol, tg, cols), BF16),
            pltpu.VMEM((rank, tg), F32),
            pltpu.VMEM((nrow, rank, tg), F32),
            pltpu.VMEM((rank, ta), F32),
            pltpu.VMEM((ncol, rank, ta), F32),
            pltpu.VMEM((nrep, rank, width), F32),
            pltpu.VMEM((nrep, rank, width), F32),
            pltpu.VMEM((rank, width), F32),
            pltpu.VMEM((nrow, rank, width), F32),
            pltpu.VMEM((nrep, rank, width), F32),
            pltpu.VMEM((ncol, rank, LANES), F32),
            pltpu.VMEM((owners, tpd, SUB, LANES), F32),
            pltpu.VMEM((nrep, tpd, SUB, LANES), F32),
            pltpu.VMEM((tpd, SUB, LANES), F32),
            pltpu.VMEM((ncol, tpd, SUB, LANES), F32),
            pltpu.VMEM((owners, tpd, SUB, LANES), F32),
            dma(CHUNKS), dma(3),
            dma(QUARTERS, nrow), dma(QUARTERS, nrow), dma(QUARTERS, ncol), dma(QUARTERS, ncol),
            dma(ncol), dma(nrow), dma(nrow), dma(ncol),
            dma(nrep), dma(nrep), dma(nrow), dma(nrow), dma(nrep), dma(nrep), dma(ncol), dma(ncol),
            dma(nrep), dma(nrep), dma(ncol), dma(ncol), dma(nrep), dma(nrep),
        ],
        compiler_params=pltpu.CompilerParams(
            collective_id=0, has_side_effects=True, vmem_limit_bytes=GRANT
        ),
        name="factors",
    )(activations, out_grads, error_buffer, right_factor.T)
    steps = 8
    new_error, new_right = pl.pallas_call(
        finish_kernel,
        out_shape=(
            jax.ShapeDtypeStruct((rows, cols), F32),
            jax.ShapeDtypeStruct((rank, cols), F32),
        ),
        in_specs=[vmem, vmem, vmem, vmem],
        out_specs=(hbm, vmem),
        scratch_shapes=[pltpu.VMEM((rows, cols), F32), dma(steps)],
        compiler_params=pltpu.CompilerParams(vmem_limit_bytes=GRANT),
        name="finish",
    )(target, los, nrs, nrt)
    return new_error, new_right.T


def body(activations, out_grads, error_buffer, right_factor):
    nrep, nrow, ncol = (lax.axis_size(a) for a in ("rep", "row", "col"))
    rows, cols = error_buffer.shape
    rank = right_factor.shape[1]
    fits = (
        nrep <= 16
        and nrow == ncol
        and activations.shape[0] % LANES == 0
        and rows % (nrep * LANES) == 0
        and rows % (8 * LANES) == 0
        and cols % LANES == 0
        and rank % 16 == 0
        and rank <= LANES
        and rows * cols * 4 <= 2**23
    )
    if not fits:
        return plain_body(activations, out_grads, error_buffer, right_factor)
    return kernel_body(nrep, nrow, ncol, activations, out_grads, error_buffer, right_factor)


def solution(mesh):
    return jax.shard_map(
        body,
        mesh=mesh,
        in_specs=(
            P(("rep", "row"), "col"),
            P(("rep", "col"), "row"),
            P(("rep", "col"), "row"),
            P("row", None),
        ),
        out_specs=(P(("rep", "col"), "row"), P("row", None)),
        check_vma=False,
    )
```

```python
import functools

import jax
import jax.numpy as jnp
from jax import lax
from jax.experimental import pallas as pl
from jax.experimental.pallas import tpu as pltpu
from jax.sharding import PartitionSpec as P

MESH = pl.DeviceIdType.MESH
F32 = jnp.float32
BF16 = jnp.bfloat16
LANES = 128
SUB = 8
CHUNKS = 4
QUARTERS = 4
GRANT = 24 * 2**20


def plain_body(activations, out_grads, error_buffer, right_factor):
    highest = lax.Precision.HIGHEST
    gathered_acts = lax.all_gather(activations, "row", axis=0, tiled=True)
    gathered_grads = lax.all_gather(out_grads, "col", axis=0, tiled=True)
    product = lax.dot_general(
        gathered_acts, gathered_grads, (((0,), (0,)), ((), ())), preferred_element_type=F32
    )
    target = product + error_buffer
    replicas = lax.axis_size("rep")
    left_part = lax.psum_scatter(
        jnp.dot(target, right_factor, precision=highest), "rep", scatter_dimension=0, tiled=True
    )
    left_part = lax.psum(left_part, "row")
    gram = lax.psum(jnp.dot(left_part.T, left_part, precision=highest), ("rep", "col"))
    lower = jnp.linalg.cholesky(gram)
    orth_part = jax.scipy.linalg.solve_triangular(lower, left_part.T, lower=True).T
    left_orth = lax.all_gather(orth_part, "rep", axis=0, tiled=True)
    right_part = lax.psum_scatter(
        lax.dot_general(
            target, left_orth, (((0,), (0,)), ((), ())), precision=highest, preferred_element_type=F32
        ),
        "rep",
        scatter_dimension=0,
        tiled=True,
    )
    right_part = lax.psum(right_part, "col") / replicas
    new_right = lax.all_gather(right_part, "rep", axis=0, tiled=True)
    approx = jnp.dot(left_orth, new_right.T, precision=highest)
    return (target - approx, new_right)


def split2(x):
    hi = x.astype(BF16)
    lo = (x - hi.astype(F32)).astype(BF16)
    return hi, lo


def dot(a, b, ca, cb, precision=None):
    return lax.dot_general(a, b, (((ca,), (cb,)), ((), ())), preferred_element_type=F32, precision=precision)


def factor_kernel(
    nrep, nrow, ncol, owners, tpd,
    acts_in, grads_in, err, right_in,
    target, los, nrs, nrt,
    e_hi, e_lo, right_t, a_all, g_all, gr_own, gr_all,
    lp, l_rx, l_own, l_row, lag, gram_all, w_tx, w_rx, w_own, w_col, wag,
    esem, loc_sem, a_ss, a_rs, g_ss, g_rs, gr_ss, gr_rs,
    l_ss, l_rs, lr_ss, lr_rs, la_ss, la_rs, gm_ss, gm_rs,
    w_ss, w_rs, wc_ss, wc_rs, wa_ss, wa_rs,
):
    rep, row, col = lax.axis_index("rep"), lax.axis_index("row"), lax.axis_index("col")
    rows, cols = target.shape
    rank = right_t.shape[0]
    chunk = rows // CHUNKS
    highest = lax.Precision.HIGHEST
    sent = []

    def remote(src, dst, ss, rs, where):
        return pltpu.make_async_remote_copy(
            src_ref=src, dst_ref=dst, send_sem=ss, recv_sem=rs, device_id=where, device_id_type=MESH
        )

    def turn(i, k, n):
        return lax.rem(i + k, n)

    barrier = pltpu.get_barrier_semaphore()
    for i in range(nrow):
        for j in range(ncol):
            if i or j:
                pl.semaphore_signal(
                    barrier, inc=1,
                    device_id={"row": turn(row, i, nrow), "col": turn(col, j, ncol)},
                    device_id_type=MESH,
                )
    for k in range(1, nrep):
        pl.semaphore_signal(barrier, inc=1, device_id={"rep": turn(rep, k, nrep)}, device_id_type=MESH)

    acts, grads = a_all.at[row], g_all.at[col]
    own_r = pltpu.make_async_copy(right_in, right_t, loc_sem.at[0])
    own_g = pltpu.make_async_copy(grads_in, grads, loc_sem.at[1])
    own_a = pltpu.make_async_copy(acts_in, acts, loc_sem.at[2])
    own_r.start()
    own_g.start()
    loads = []
    for c in range(CHUNKS):
        part = pl.ds(c * chunk, chunk)
        loads.append(pltpu.make_async_copy(err.at[part], target.at[part], esem.at[c]))
        loads[-1].start()
    own_a.start()
    own_r.wait()
    own_g.wait()
    r_hi, r_lo = split2(right_t[...])
    r_two = jnp.concatenate([r_hi, r_lo], axis=0)
    gr2 = dot(r_two, grads[...], 1, 1)
    gr_own[...] = gr2[:rank] + gr2[rank:]

    pieces = []

    def error_term(c):
        loads[c].wait()
        part = pl.ds(c * chunk, chunk)
        hi, lo = split2(target[part, :])
        e_hi[part, :] = hi
        e_lo[part, :] = lo
        two = dot(r_two, hi, 1, 1)
        pieces.append(two[:rank] + two[rank:] + dot(r_hi, lo, 1, 1))

    early = CHUNKS // 2
    for c in range(early):
        error_term(c)
    own_a.wait()

    pl.semaphore_wait(barrier, nrep - 1 + nrow * ncol - 1)

    gr_copies = []
    for j in range(ncol):
        cp = remote(gr_own, gr_all.at[row], gr_ss.at[j], gr_rs.at[row], {"row": col, "col": j})
        is_self = jnp.logical_and(row == col, col == j)
        gr_copies.append((cp, is_self))

        @pl.when(jnp.logical_not(is_self))
        def _():
            cp.start()

    @pl.when(row == col)
    def _():
        gr_all[row] = gr_own[...]

    ta, tg = acts.shape[0] // QUARTERS, grads.shape[0] // QUARTERS
    bulk = []
    for q in range(QUARTERS):
        for k in range(1, nrow):
            s = pl.ds(q * ta, ta)
            bulk.append(remote(a_all.at[row, s], a_all.at[row, s], a_ss.at[q, k], a_rs.at[q, k], {"row": turn(row, k, nrow)}))
        for k in range(1, ncol):
            s = pl.ds(q * tg, tg)
            bulk.append(remote(g_all.at[col, s], g_all.at[col, s], g_ss.at[q, k], g_rs.at[q, k], {"col": turn(col, k, ncol)}))
    per = nrow + ncol - 2
    for cp in bulk[:2 * per]:
        cp.start()

    for c in range(early, CHUNKS):
        error_term(c)
    for i in range(nrow):
        @pl.when(jnp.logical_not(jnp.logical_and(row == col, row == i)))
        def _():
            remote(gr_own, gr_all.at[i], gr_ss.at[0], gr_rs.at[i], {"row": col}).wait_recv()
    gr = gr_all[0]
    for i in range(1, nrow):
        gr = gr + gr_all[i]
    gr_hi, gr_lo = split2(gr)
    two = dot(jnp.concatenate([gr_hi, gr_lo], axis=0), acts[...], 1, 0)
    part_left = jnp.concatenate(pieces, axis=1) + two[:rank] + two[rank:]
    width = rows // nrep
    for k in range(nrep):
        lp[k] = part_left[:, k * width:(k + 1) * width]

    copies = []
    for k in range(1, nrep):
        to = turn(rep, k, nrep)
        cp = remote(lp.at[to], l_rx.at[rep], l_ss.at[k], l_rs.at[k], {"rep": to})
        cp.start()
        copies.append(cp)
    sent += copies
    total = lp[rep]
    for k, cp in enumerate(copies, 1):
        cp.wait_recv()
        total = total + l_rx[turn(rep, nrep - k, nrep)]
    l_own[...] = total
    copies = []
    for k in range(1, nrow):
        cp = remote(l_own, l_row.at[row], lr_ss.at[k], lr_rs.at[k], {"row": turn(row, k, nrow)})
        cp.start()
        copies.append(cp)
    sent += copies
    for cp in bulk[2 * per:]:
        cp.start()
    l_row[row] = total
    for cp in copies:
        cp.wait_recv()
    total = l_row[0]
    for i in range(1, nrow):
        total = total + l_row[i]
    lag[rep] = total
    copies = []
    for k in range(1, nrep):
        cp = remote(lag.at[rep], lag.at[rep], la_ss.at[k], la_rs.at[k], {"rep": turn(rep, k, nrep)})
        cp.start()
        copies.append(cp)
    sent += copies
    for cp in copies:
        cp.wait_recv()
    left = jnp.concatenate([lag[k] for k in range(nrep)], axis=1)
    l_hi, l_lo = split2(left)
    l_two = jnp.concatenate([l_hi, l_lo], axis=0)

    gram_all[col] = jnp.zeros(gram_all.shape[1:], F32)
    gram_all[col, :, 0:rank] = dot(left, left, 1, 1, highest)
    gram_copies = []
    for k in range(1, ncol):
        cp = remote(gram_all.at[col], gram_all.at[col], gm_ss.at[k], gm_rs.at[k], {"col": turn(col, k, ncol)})
        cp.start()
        gram_copies.append(cp)
    sent += gram_copies

    two = dot(l_two, e_hi[...], 1, 0)
    w = two[:rank] + two[rank:] + dot(l_hi, e_lo[...], 1, 0)
    for cp in bulk:
        cp.wait_recv()
    a_full = a_all[...].reshape(nrow * acts_in.shape[0], rows)
    g_full = g_all[...].reshape(ncol * grads_in.shape[0], cols)
    la2 = dot(l_two, a_full, 1, 1)
    la_hi, la_lo = split2(la2[:rank] + la2[rank:])
    two = dot(jnp.concatenate([la_hi, la_lo], axis=0), g_full, 1, 0)
    w = w + two[:rank] + two[rank:]
    lane_tiles = cols // LANES
    tiles = (rank // SUB) * lane_tiles
    for t in range(owners * tpd):
        if t < tiles:
            h, l = divmod(t, lane_tiles)
            w_tx[t // tpd, t % tpd] = w[h * SUB:(h + 1) * SUB, l * LANES:(l + 1) * LANES]
        else:
            w_tx[t // tpd, t % tpd] = jnp.zeros((SUB, LANES), F32)

    copies = []
    for k in range(1, nrep):
        to = turn(rep, k, nrep)
        keep = to < owners
        slot = jnp.minimum(to, owners - 1)
        cp = remote(w_tx.at[slot], w_rx.at[rep], w_ss.at[k], w_rs.at[k], {"rep": to})
        copies.append((cp, keep))

        @pl.when(keep)
        def _():
            cp.start()

    for cp in gram_copies:
        cp.wait_recv()
    gram = gram_all[0]
    for j in range(1, ncol):
        gram = gram + gram_all[j]
    gram = gram[:, 0:rank]
    ri = lax.broadcasted_iota(jnp.int32, (rank, rank), 0)
    ci = lax.broadcasted_iota(jnp.int32, (rank, rank), 1)
    r1 = lax.broadcasted_iota(jnp.int32, (rank, 1), 0)
    inv = jnp.where(ri == ci, 1.0, 0.0).astype(F32)
    for j in range(rank):
        f = jnp.where(r1 > j, gram[:, j:j + 1] / gram[j:j + 1, j:j + 1], 0.0)
        inv = inv - f * inv[j:j + 1, :]
        gram = gram - f * gram[j:j + 1, :]
    diag = jnp.sum(jnp.where(ri == ci, gram, 0.0), axis=1, keepdims=True)
    inv = inv / jnp.sqrt(diag)

    mine = rep < owners
    own_slot = jnp.minimum(rep, owners - 1)
    ex = [
        remote(w_own, w_col.at[col], wc_ss.at[k], wc_rs.at[k], {"col": turn(col, k, ncol)})
        for k in range(1, ncol)
    ]
    gather = [
        remote(wag.at[own_slot], wag.at[own_slot], wa_ss.at[k], wa_rs.at[k], {"rep": turn(rep, k, nrep)})
        for k in range(1, nrep)
    ]

    @pl.when(mine)
    def _():
        total = w_tx[own_slot]
        for k, (cp, keep) in enumerate(copies, 1):
            cp.wait_recv()
            total = total + w_rx[turn(rep, nrep - k, nrep)]
        w_own[...] = total
        w_col[col] = total
        for cp in ex:
            cp.start()

    def target_term(c):
        part = pl.ds(c * chunk, chunk)
        a = a_all[:, :, c * chunk:(c + 1) * chunk].reshape(nrow * acts.shape[0], chunk)
        g = g_all[...].reshape(ncol * grads.shape[0], cols)
        target[part, :] = dot(a, g, 0, 0) + target[part, :]

    for c in range(early):
        target_term(c)

    @pl.when(mine)
    def _():
        for cp in ex:
            cp.wait_recv()
        total = w_col[0]
        for j in range(1, ncol):
            total = total + w_col[j]
        wag[own_slot] = total
        for cp in gather:
            cp.start()

    lo_t = dot(inv, left, 1, 0, highest)
    o_hi, o_lo = split2(lo_t)
    los[...] = jnp.concatenate([o_hi, o_hi, o_lo], axis=0)
    for c in range(early, CHUNKS):
        target_term(c)

    for k in range(1, nrep):
        @pl.when(turn(rep, nrep - k, nrep) < owners)
        def _():
            gather[k - 1].wait_recv()
    halves = []
    for h in range(rank // SUB):
        ts = [h * lane_tiles + l for l in range(lane_tiles)]
        halves.append(jnp.concatenate([wag[t // tpd, t % tpd] for t in ts], axis=1))
    w_all = jnp.concatenate(halves, axis=0)
    nr = dot(inv, w_all, 1, 0, highest) / nrep
    nrt[...] = nr
    n_hi, n_lo = split2(nr)
    nrs[...] = jnp.concatenate([n_hi, n_lo, n_hi], axis=0)

    for cp, is_self in gr_copies:
        @pl.when(jnp.logical_not(is_self))
        def _():
            cp.wait_send()
    for cp in sent + bulk:
        cp.wait_send()
    for cp, keep in copies:
        @pl.when(keep)
        def _():
            cp.wait_send()

    @pl.when(mine)
    def _():
        for cp in ex + gather:
            cp.wait_send()


def finish_kernel(t, los, nrs, nrt, out, right_out, buf, sem):
    rows = t.shape[0]
    steps = sem.shape[0]
    block = rows // steps
    stores = []
    for c in range(steps):
        part = pl.ds(c * block, block)
        buf[part, :] = t[part, :] - dot(los[:, c * block:(c + 1) * block], nrs[...], 0, 0)
        stores.append(pltpu.make_async_copy(buf.at[part], out.at[part], sem.at[c]))
        stores[-1].start()
    right_out[...] = nrt[...]
    for cp in stores:
        cp.wait()


def kernel_body(nrep, nrow, ncol, activations, out_grads, error_buffer, right_factor):
    rows, cols = error_buffer.shape
    rank = right_factor.shape[1]
    ta, tg = activations.shape[0], out_grads.shape[0]
    tiles = (rank // SUB) * (cols // LANES)
    tpd = -(-tiles // nrep)
    owners = -(-tiles // tpd)
    width = rows // nrep
    vmem = pl.BlockSpec(memory_space=pltpu.VMEM)
    hbm = pl.BlockSpec(memory_space=pltpu.HBM)
    dma = lambda *s: pltpu.SemaphoreType.DMA(s)
    target, los, nrs, nrt = pl.pallas_call(
        functools.partial(factor_kernel, nrep, nrow, ncol, owners, tpd),
        out_shape=(
            pltpu.VMEM((rows, cols), F32),
            pltpu.VMEM((3 * rank, rows), BF16),
            pltpu.VMEM((3 * rank, cols), BF16),
            pltpu.VMEM((rank, cols), F32),
        ),
        in_specs=[hbm] * 4,
        out_specs=(vmem, vmem, vmem, vmem),
        scratch_shapes=[
            pltpu.VMEM((rows, cols), BF16),
            pltpu.VMEM((rows, cols), BF16),
            pltpu.VMEM((rank, cols), F32),
            pltpu.VMEM((nrow, ta, rows), BF16),
            pltpu.VMEM((ncol, tg, cols), BF16),
            pltpu.VMEM((rank, tg), F32),
            pltpu.VMEM((nrow, rank, tg), F32),
            pltpu.VMEM((nrep, rank, width), F32),
            pltpu.VMEM((nrep, rank, width), F32),
            pltpu.VMEM((rank, width), F32),
            pltpu.VMEM((nrow, rank, width), F32),
            pltpu.VMEM((nrep, rank, width), F32),
            pltpu.VMEM((ncol, rank, LANES), F32),
            pltpu.VMEM((owners, tpd, SUB, LANES), F32),
            pltpu.VMEM((nrep, tpd, SUB, LANES), F32),
            pltpu.VMEM((tpd, SUB, LANES), F32),
            pltpu.VMEM((ncol, tpd, SUB, LANES), F32),
            pltpu.VMEM((owners, tpd, SUB, LANES), F32),
            dma(CHUNKS), dma(3),
            dma(QUARTERS, nrow), dma(QUARTERS, nrow), dma(QUARTERS, ncol), dma(QUARTERS, ncol),
            dma(ncol), dma(nrow),
            dma(nrep), dma(nrep), dma(nrow), dma(nrow), dma(nrep), dma(nrep), dma(ncol), dma(ncol),
            dma(nrep), dma(nrep), dma(ncol), dma(ncol), dma(nrep), dma(nrep),
        ],
        compiler_params=pltpu.CompilerParams(
            collective_id=0, has_side_effects=True, vmem_limit_bytes=GRANT
        ),
        name="factors",
    )(*(pltpu.with_memory_space_constraint(x, pltpu.HBM) for x in (activations, out_grads, error_buffer, right_factor.T)))
    steps = 8
    new_error, new_right = pl.pallas_call(
        finish_kernel,
        out_shape=(
            jax.ShapeDtypeStruct((rows, cols), F32),
            jax.ShapeDtypeStruct((rank, cols), F32),
        ),
        in_specs=[vmem, vmem, vmem, vmem],
        out_specs=(hbm, vmem),
        scratch_shapes=[pltpu.VMEM((rows, cols), F32), dma(steps)],
        compiler_params=pltpu.CompilerParams(vmem_limit_bytes=GRANT),
        name="finish",
    )(target, los, nrs, nrt)
    return new_error, new_right.T


def body(activations, out_grads, error_buffer, right_factor):
    nrep, nrow, ncol = (lax.axis_size(a) for a in ("rep", "row", "col"))
    rows, cols = error_buffer.shape
    rank = right_factor.shape[1]
    fits = (
        nrep <= 16
        and nrow == ncol
        and activations.shape[0] % LANES == 0
        and rows % (nrep * LANES) == 0
        and rows % (8 * LANES) == 0
        and cols % LANES == 0
        and rank % 16 == 0
        and rank <= LANES
        and rows * cols * 4 <= 2**23
    )
    if not fits:
        return plain_body(activations, out_grads, error_buffer, right_factor)
    return kernel_body(nrep, nrow, ncol, activations, out_grads, error_buffer, right_factor)


def solution(mesh):
    return jax.shard_map(
        body,
        mesh=mesh,
        in_specs=(
            P(("rep", "row"), "col"),
            P(("rep", "col"), "row"),
            P(("rep", "col"), "row"),
            P("row", None),
        ),
        out_specs=(P(("rep", "col"), "row"), P("row", None)),
        check_vma=False,
    )
```
